32 devices in a mesh: dp: 4 (over x, core), mp: 8 (over z, y).
Axes of the slice: x: 2, y: 2, z: 4, core: 2. Of those that a mesh axis runs over, the one named last changes fastest.
Arguments:
- tokens: bfloat16 [1024, 8192], P('dp'), may hold values from -6 to 6
- norm_gain: float32 [8192], replicated, may hold values from 0.5 to 1.5
- gate_weight: bfloat16 [8192, 28672], P('dp', 'mp'), may hold values from -0.0625 to 0.0625
- gate_mask: int32 [8192, 896], P('dp', 'mp'), may hold values from -2147483648 to 2147483646
- up_weight: bfloat16 [8192, 28672], P('dp', 'mp'), may hold values from -0.0625 to 0.0625
- up_mask: int32 [8192, 896], P('dp', 'mp'), may hold values from -2147483648 to 2147483646
- down_weight: bfloat16 [28672, 8192], P('mp', 'dp'), may hold values from -0.03125 to 0.03125
- down_mask: int32 [28672, 256], P('mp', 'dp'), may hold values from -2147483648 to 2147483647, as said below
Outputs:
- mixed: bfloat16 [1024, 8192], P('mp', 'dp')
- input_norms: float32 [8192], P('dp')
- hidden_norms: float32 [28672], P('mp')
The draws below stay inside these ranges and needn't reach their ends.
Inputs may be any that keep to these rules, and one draw needn't show every extreme that they name: `down_mask`: in every word each of the eight aligned groups of four bits holds exactly two ones, so exactly two of every four consecutive columns of the down projection are kept.
All inputs are finite; a program needn't handle non-finite values.
Results may differ from the reference program's by a relative error of at most 0.025.
Values may be sent and summed in bfloat16 or wider, within the bound.
A program may use at most 192 MiB of HBM per device.

```python
import jax
import jax.numpy as jnp
from jax import lax

D = 8192
FF = 28672
TOKENS = 1024
N_DP = 4
N_MP = 8


def draw_down_mask(key, part):
    patterns = jnp.array([3, 5, 6, 9, 10, 12], jnp.int32)
    selected = jax.random.randint(key, (FF, D // 32, 8), 0, 6, dtype=jnp.int32)
    nibbles = patterns[selected]
    shifts = 4 * jnp.arange(8, dtype=jnp.int32)
    placed = jnp.left_shift(nibbles, shifts)
    return jnp.sum(placed, axis=2, dtype=jnp.int32)


def set_ends(entries, rng, least, largest):
    longest = entries.shape.index(max(entries.shape))
    spots = []
    for shift in (0, 1):
        where = [jax.random.randint(jax.random.fold_in(rng, axis), (), 0, length) for axis, length in enumerate(entries.shape)]
        where[longest] = (where[longest] + shift) % entries.shape[longest]
        spots.append(tuple(where))
    return entries.at[spots[0]].set(least).at[spots[1]].set(largest)


def level_of(key, shape, split, smallest, high):
    def one(axis_at, blocks):
        heights = jax.random.uniform(jax.random.fold_in(jax.random.fold_in(key, 6), axis_at), (blocks,), jnp.float32, smallest / len(split), high / len(split))
        return jnp.repeat(jnp.exp(heights), shape[axis_at] // blocks).reshape((-1,) + (1,) * (len(shape) - axis_at - 1))

    level = one(*split[0])
    for cut in split[1:]:
        level = level * one(*cut)
    return level


def centred(stream_key, extent, width, most, cuts=(), kind=jnp.bfloat16):
    gain = level_of(stream_key, extent, cuts, -0.22, 0.18) if cuts else 1.0
    entries = jax.random.normal(stream_key, extent, jnp.float32) * width * gain
    return jnp.minimum(jnp.maximum(entries, -most), most).astype(kind)


def setup_inputs(seed: int = 0) -> dict:
    keys = jax.random.split(jax.random.key(seed), 9)
    tokens = centred(keys[0], (TOKENS, D), 1.0, 6.0, ((0, 4),))
    norm_gain = jnp.clip(1.0 + 0.1 * jax.random.normal(keys[1], (D,), jnp.float32), 0.5, 1.5)
    gate_weight = centred(keys[2], (D, FF), D ** -0.5, 0.0625, ((0, 4), (1, 8)))
    gate_mask = set_ends(jax.random.randint(keys[3], (D, FF // 32), -2147483648, 2147483647), jax.random.fold_in(keys[3], 1), -2147483648, 2147483646).astype(jnp.int32)
    up_weight = centred(keys[4], (D, FF), D ** -0.5, 0.0625, ((0, 4), (1, 8)))
    up_mask = set_ends(jax.random.randint(keys[5], (D, FF // 32), -2147483648, 2147483647), jax.random.fold_in(keys[5], 1), -2147483648, 2147483646).astype(jnp.int32)
    down_weight = centred(keys[6], (FF, D), FF ** -0.5, 0.03125, ((0, 8), (1, 4)))
    down_mask = draw_down_mask(jax.random.fold_in(keys[8], 71), 0)
    return dict(tokens=tokens, norm_gain=norm_gain, gate_weight=gate_weight, gate_mask=gate_mask, up_weight=up_weight, up_mask=up_mask, down_weight=down_weight, down_mask=down_mask)


def keep_entries(weight, packed):
    shifts = jnp.arange(32, dtype=jnp.int32)
    kept_bits = jnp.right_shift(packed[..., None], shifts) & 1
    kept_bits = kept_bits.reshape(weight.shape)
    return jnp.where(kept_bits == 1, weight, jnp.zeros_like(weight))

def reference(tokens, norm_gain, gate_weight, gate_mask, up_weight, up_mask, down_weight, down_mask):
    values = tokens.astype(jnp.float32)
    scale = lax.rsqrt(lax.optimization_barrier(jnp.mean(values * values, axis=1, keepdims=True)) + 1e-05)
    normed = (values * scale * norm_gain).astype(jnp.bfloat16)
    widened = normed.astype(jnp.float32)
    input_norms = jnp.sqrt(lax.optimization_barrier(jnp.sum(widened * widened, axis=0)))
    stride = D // N_DP

    def add_block(position, sums_so_far):
        gate_sum, up_sum = sums_so_far
        offset = (position * stride).astype(jnp.int32)
        row_block = lax.dynamic_slice_in_dim(normed, offset, stride, 1)
        gate_rows = keep_entries(lax.dynamic_slice_in_dim(gate_weight, offset, stride, 0), lax.dynamic_slice_in_dim(gate_mask, offset, stride, 0))
        up_rows = keep_entries(lax.dynamic_slice_in_dim(up_weight, offset, stride, 0), lax.dynamic_slice_in_dim(up_mask, offset, stride, 0))
        gate_part = jnp.dot(row_block, gate_rows, preferred_element_type=jnp.float32).astype(jnp.bfloat16)
        up_part = jnp.dot(row_block, up_rows, preferred_element_type=jnp.float32).astype(jnp.bfloat16)
        gate_part, up_part = lax.optimization_barrier((gate_part, up_part))
        return (gate_sum + gate_part.astype(jnp.float32), up_sum + up_part.astype(jnp.float32))
    zeros_sum = jnp.zeros((normed.shape[0], FF), jnp.float32)
    gate, up = lax.fori_loop(0, N_DP, add_block, (zeros_sum, zeros_sum))
    hidden = (jax.nn.silu(gate) * up).astype(jnp.bfloat16)
    wide_hidden = hidden.astype(jnp.float32)
    hidden_norms = jnp.sqrt(lax.optimization_barrier(jnp.sum(wide_hidden * wide_hidden, axis=0)))
    unit_stride = FF // N_MP

    def add_down(position, running):
        offset = (position * unit_stride).astype(jnp.int32)
        row_block = lax.dynamic_slice_in_dim(hidden, offset, unit_stride, 1)
        down_rows = keep_entries(lax.dynamic_slice_in_dim(down_weight, offset, unit_stride, 0), lax.dynamic_slice_in_dim(down_mask, offset, unit_stride, 0))
        return running + jnp.dot(row_block, down_rows, preferred_element_type=jnp.float32)
    mixed = lax.fori_loop(0, N_MP, add_down, jnp.zeros((normed.shape[0], D), jnp.float32))
    return (mixed.astype(jnp.bfloat16), input_norms, hidden_norms)
```

```python
import jax
import jax.numpy as jnp
from jax import lax
from jax.experimental import pallas as pl
from jax.experimental.pallas import tpu as pltpu
from jax.sharding import PartitionSpec as P

CORES = 2
CHUNKS = 4
GROUPS = 2


def mask_kernel(weight_ref, words_ref, kept_ref):
    rows, columns = weight_ref.shape
    lanes = lax.broadcasted_iota(jnp.int32, (rows, 128), 1)
    shifts = 31 - lanes % 32
    word = lanes // 32
    for group in range(columns // 128):
        first = 4 * group
        slab = words_ref[:, first // 128 * 128 : first // 128 * 128 + 128]
        spread = jnp.take_along_axis(slab, word + first % 128, axis=1)
        kept = jnp.left_shift(spread, shifts) < 0
        span = slice(128 * group, 128 * group + 128)
        values = weight_ref[:, span].astype(jnp.float32)
        kept_ref[:, span] = jnp.where(kept, values, 0.0).astype(jnp.bfloat16)


def keep_entries(weight, packed):
    rows, columns = weight.shape
    padded = -(-packed.shape[1] // 128) * 128
    words = jnp.pad(packed, ((0, 0), (0, padded - packed.shape[1])))
    block = 128
    return pl.pallas_call(
        mask_kernel,
        grid=(rows // block,),
        in_specs=[
            pl.BlockSpec((block, columns), lambda i: (i, 0)),
            pl.BlockSpec((block, padded), lambda i: (i, 0)),
        ],
        out_specs=pl.BlockSpec((block, columns), lambda i: (i, 0)),
        out_shape=jax.ShapeDtypeStruct(weight.shape, weight.dtype),
        cost_estimate=pl.CostEstimate(
            flops=4 * rows * columns, bytes_accessed=5 * rows * columns, transcendentals=0
        ),
    )(weight, words)


def tie_kernel(value_ref, earlier_ref, out_ref):
    pass


def tie(value, earlier):
    return pl.pallas_call(
        tie_kernel,
        in_specs=[pl.BlockSpec(memory_space=pl.ANY)] * 2,
        out_specs=pl.BlockSpec(memory_space=pl.ANY),
        out_shape=jax.ShapeDtypeStruct(value.shape, value.dtype),
        input_output_aliases={0: 0},
    )(value, earlier)


def norm_kernel(tokens_ref, gain_ref, normed_ref):
    values = tokens_ref[...].astype(jnp.float32)
    scale = lax.rsqrt(jnp.mean(values * values, axis=1, keepdims=True) + 1e-05)
    normed_ref[...] = (values * scale * gain_ref[...]).astype(jnp.bfloat16)


def normalise(tokens, norm_gain, shards):
    rows, features = tokens.shape
    block = rows // (shards * CHUNKS)
    return pl.pallas_call(
        norm_kernel,
        grid=(shards * CHUNKS,),
        in_specs=[
            pl.BlockSpec((block, features), lambda i: ((i % shards) * CHUNKS + i // shards, 0)),
            pl.BlockSpec((1, features), lambda i: (0, 0)),
        ],
        out_specs=pl.BlockSpec((block, features), lambda i: (i, 0)),
        out_shape=jax.ShapeDtypeStruct(tokens.shape, jnp.bfloat16),
        cost_estimate=pl.CostEstimate(
            flops=5 * rows * features, bytes_accessed=4 * rows * features, transcendentals=rows
        ),
    )(tokens, norm_gain[None, :])


def on_device(
    n_dp, n_mp,
    tokens, norm_gain, gate_weight, gate_mask, up_weight, up_mask, down_weight, down_mask
):
    chips = n_dp // CORES
    position = lax.axis_index("dp")
    chip, core = position // CORES, position % CORES
    rows = tokens.shape[0]
    width = gate_weight.shape[0]
    units = gate_weight.shape[1]
    small = rows // CHUNKS

    def across(value, shift):
        pairs = [
            (d, (d // CORES + shift) % chips * CORES + d % CORES) for d in range(n_dp)
        ]
        return lax.ppermute(value, "dp", pairs)

    def to_partner(value):
        return lax.ppermute(value, "dp", [(d, d ^ 1) for d in range(n_dp)])

    def by_core(mine, other, axis):
        first = jnp.where(core == 0, mine, other)
        second = jnp.where(core == 0, other, mine)
        return jnp.stack([first, second], axis=axis)

    normed = normalise(tokens, norm_gain, n_mp // n_dp)

    def chip_columns(which, source):
        return lax.dynamic_slice_in_dim(source, which * CORES * width, CORES * width, 1)

    def share(block):
        mine = lax.dynamic_slice_in_dim(block, core * width, width, 1)
        theirs = lax.dynamic_slice_in_dim(block, (1 - core) * width, width, 1)
        other = to_partner(theirs)
        shape = (CHUNKS, small, width)
        return by_core(mine.reshape(shape), other.reshape(shape), 1)

    gate_kept = keep_entries(gate_weight, gate_mask)
    up_kept = keep_entries(up_weight, up_mask)
    columns = []
    for shift in range(1, chips):
        landed = across(chip_columns((chip + shift) % chips, normed), shift)
        columns.append(share(tie(tie(landed, gate_kept), up_kept)))
    own_columns = share(chip_columns(chip, normed))


    def pair_sums(block, gate_kept, up_kept):
        count = block.shape[0]
        flat = block.reshape(-1, width)
        halves = []
        for kept in (gate_kept, up_kept):
            part = jnp.dot(flat, kept, preferred_element_type=jnp.float32).astype(jnp.bfloat16)
            part = part.reshape(count, CORES, small, units)
            mine = lax.dynamic_index_in_dim(part, core, 1, keepdims=False)
            theirs = lax.dynamic_index_in_dim(part, 1 - core, 1, keepdims=False)
            other = to_partner(theirs)
            halves.append(mine.astype(jnp.float32) + other.astype(jnp.float32))
        return halves

    grouped = CHUNKS // GROUPS
    arrived = [[] for _ in range(CHUNKS)]
    both = None
    for group in range(GROUPS):
        for shift in range(1, chips):
            block = columns[shift - 1][group * grouped : (group + 1) * grouped]
            if both is not None:
                block = tie(block, both)
            gate_sum, up_sum = pair_sums(block, gate_kept, up_kept)
            both = jnp.concatenate([gate_sum, up_sum], axis=2).astype(jnp.bfloat16)
            for inner in range(grouped):
                arrived[group * grouped + inner].append(across(both[inner], -shift))
    if both is not None:
        down_mask = tie(down_mask, both)
    down_kept = keep_entries(down_weight, down_mask)
    late_columns = tie(own_columns, down_kept)
    own_gate, own_up = pair_sums(late_columns, gate_kept, up_kept)

    def scatter_sums(partial):
        left = partial.reshape(n_mp, -1, partial.shape[1])
        place = lax.axis_index("mp")
        step = 1
        while step < n_mp:
            halves = left.reshape((-1, 2) + left.shape[1:])
            bit = place // step % 2
            mine = lax.dynamic_index_in_dim(halves, bit, 1, keepdims=False)
            theirs = lax.dynamic_index_in_dim(halves, 1 - bit, 1, keepdims=False)
            other = lax.ppermute(theirs, "mp", [(m, m ^ step) for m in range(n_mp)])
            left = (mine.astype(jnp.float32) + other.astype(jnp.float32)).astype(jnp.bfloat16)
            step *= 2
        return left[0]

    squares = jnp.zeros((units,), jnp.float32)
    outs = []
    for chunk in range(CHUNKS):
        gate, up = own_gate[chunk], own_up[chunk]
        for value in arrived[chunk]:
            gate = gate + value[:, :units].astype(jnp.float32)
            up = up + value[:, units:].astype(jnp.float32)
        hidden = (jax.nn.silu(gate) * up).astype(jnp.bfloat16)
        pieces = [hidden] + [across(hidden, shift) for shift in range(1, chips)]
        stack = jnp.stack(pieces)
        both_cores = by_core(stack, to_partner(stack), 1)
        whole = jnp.concatenate(
            [
                lax.dynamic_index_in_dim(both_cores, (chip - g) % chips, 0, keepdims=False)
                for g in range(chips)
            ]
        ).reshape(-1, units)
        wide = whole.astype(jnp.float32)
        squares = squares + jnp.sum(wide * wide, axis=0)
        partial_out = jnp.dot(whole, down_kept, preferred_element_type=jnp.float32)
        outs.append(scatter_sums(partial_out.astype(jnp.bfloat16)))
    mixed = jnp.concatenate(outs, axis=0)
    hidden_norms = jnp.sqrt(squares)

    totals = jnp.zeros((width,), jnp.float32)
    for block in columns + [own_columns]:
        widened = block.astype(jnp.float32)
        totals = totals + jnp.sum(widened * widened, axis=(0, 1, 2))
    return (mixed, jnp.sqrt(totals), hidden_norms)


def solution(mesh):
    n_dp, n_mp = mesh.shape["dp"], mesh.shape["mp"]

    def body(*args):
        return on_device(n_dp, n_mp, *args)

    return jax.shard_map(
        body,
        mesh=mesh,
        in_specs=(
            P("dp", None),
            P(),
            P("dp", "mp"),
            P("dp", "mp"),
            P("dp", "mp"),
            P("dp", "mp"),
            P("mp", "dp"),
            P("mp", "dp"),
        ),
        out_specs=(P("mp", "dp"), P("dp"), P("mp")),
        check_vma=False,
    )
```
